32 devices in a mesh: queue: 8 (over z, y), batch: 4 (over x, core).
Axes of the slice: x: 2, y: 2, z: 4, core: 2. Of those that a mesh axis runs over, the one named last changes fastest.
Arguments:
- queries: bfloat16 [4096, 256], P(('queue', 'batch')), may hold values from -160 to 160
- keys: bfloat16 [4096, 256], P(('queue', 'batch')), may hold values from -0.5 to 0.5
- queue_keys: bfloat16 [32768, 256], P('queue'), may hold values from -2 to 2
- log_scale: float32 [1], replicated, may hold values from 0 to 1
- write_pointer: int32 [1], replicated, may hold values from 0 to 255
- block_order: int32 [32], replicated, may hold values from 0 to 31, each once
- pos_index: int32 [4096], P(('queue', 'batch')), may hold values from 0 to 127
Outputs:
- loss: float32 [4096], P(('queue', 'batch'))
- temp_grad: float32 [1], replicated
- new_queue: bfloat16 [32768, 256], P('queue')
The draws below stay inside these ranges and needn't reach their ends.
Inputs may be any that keep to these rules, and one draw needn't show every extreme that they name: `block_order`: each number of 0 to 31 appears once.
All inputs are finite; a program needn't handle non-finite values.
Results may differ from the reference program's by a relative error of at most 0.0004.
Values may be sent and summed in bfloat16 or wider, within the bound.
No kernel may reach another device: no remote copies, remote signals or barrier semaphores. Data moves between devices by JAX's collectives and lax.ppermute only.
A program may use at most 64 MiB of HBM per device.

```python
import jax
import jax.numpy as jnp
from jax import lax

D = 256
BLOCK = 128
TOK_DEV = 128
B = 4096
QUEUE = 32768
NEWBLK = 32
QBLOCKS = 256


def shared_queue(key):
    base = jax.random.normal(jax.random.fold_in(key, 11), (QUEUE, D), jnp.float32)
    base = jnp.clip(base, -8.0, 8.0) * 0.0625
    return base


def draw_queue_keys(key, part):
    return shared_queue(key).astype(jnp.bfloat16)


def draw_queries(key, part):
    base = jnp.clip(jax.random.normal(jax.random.fold_in(key, 21), (B, D), jnp.float32), -6.0, 6.0)
    return base.astype(jnp.bfloat16)


def touch_ends(drawn, rng, smallest, top_value):
    dims = drawn.shape
    place = [jax.random.randint(jax.random.fold_in(rng, axis), (), 0, dims[axis]) for axis in range(len(dims))]
    drawn = drawn.at[tuple(place)].set(smallest)
    longest = dims.index(max(dims))
    place[longest] = (place[longest] + 1) % dims[longest]
    return drawn.at[tuple(place)].set(top_value)


def block_scale(own_key, dims, split, smallest, high):
    def one(axis_at, parts):
        heights = jax.random.uniform(jax.random.fold_in(jax.random.fold_in(own_key, 6), axis_at), (parts,), jnp.float32, smallest / len(split), high / len(split))
        return jnp.repeat(jnp.exp(heights), dims[axis_at] // parts).reshape((-1,) + (1,) * (len(dims) - axis_at - 1))

    level = one(*split[0])
    for cut in split[1:]:
        level = level * one(*cut)
    return level


def gaussian(own_key, extent, scale, reach, pieces=(), held_as=jnp.bfloat16):
    entries = scale * jax.random.normal(own_key, extent, jnp.float32)
    if pieces:
        entries = entries * block_scale(own_key, extent, pieces, -0.22, 0.18)
    return jnp.clip(entries, -reach, reach).astype(held_as)


def setup_inputs(seed: int = 0) -> dict:
    splits = jax.random.split(jax.random.key(seed), 8)
    queries = draw_queries(jax.random.fold_in(splits[7], 71), 0)
    keys = gaussian(splits[1], (B, D), 0.0625, 0.5, ((0, 32),))
    queue_keys = draw_queue_keys(jax.random.fold_in(splits[7], 71), 0)
    log_scale = jnp.clip(jax.random.uniform(splits[3], (1,), jnp.float32, 0.0, 1.0), 0.0, 1.0)
    write_pointer = jax.random.randint(splits[4], (1,), 0, QBLOCKS).astype(jnp.int32)
    block_order = jax.random.permutation(splits[5], NEWBLK).astype(jnp.int32)
    pos_index = touch_ends(jax.random.randint(splits[6], (B,), 0, TOK_DEV), jax.random.fold_in(splits[6], 1), 0, TOK_DEV - 1).astype(jnp.int32)
    return dict(queries=queries, keys=keys, queue_keys=queue_keys, log_scale=log_scale, write_pointer=write_pointer, block_order=block_order, pos_index=pos_index)


def block_stats(query_block, queue_keys, scale):
    logits = scale * jnp.dot(query_block, queue_keys.T, preferred_element_type=jnp.float32)
    highest = jnp.max(logits, axis=1)
    weights = jnp.exp(logits - highest[:, None])
    return highest, jnp.sum(weights, axis=1), jnp.sum(weights * logits, axis=1)


def reference(queries, keys, queue_keys, log_scale, write_pointer, block_order, pos_index):
    scale = jnp.exp(log_scale[0])
    total_rows = queries.shape[0]
    groups = total_rows // TOK_DEV
    grouped_q = queries.reshape(groups, TOK_DEV, D).astype(jnp.float32)
    grouped_k = keys.reshape(groups, TOK_DEV, D).astype(jnp.float32)
    local_scores = jnp.einsum("gtd,gsd->gts", grouped_q, grouped_k)
    picked = jnp.take_along_axis(local_scores, pos_index.reshape(groups, TOK_DEV, 1).astype(jnp.int32), axis=2)
    pos = scale * picked.reshape(total_rows)
    width = min(512, total_rows)
    blocks = queries.reshape(total_rows // width, width, D)
    peak, total, weighted = lax.map(lambda block_rows: block_stats(block_rows, queue_keys, scale), blocks)
    peak = peak.reshape(total_rows)
    total = total.reshape(total_rows)
    weighted = weighted.reshape(total_rows)
    highest = jnp.maximum(peak, pos)
    factor = jnp.exp(peak - highest)
    own_weight = jnp.exp(pos - highest)
    final_total = total * factor + own_weight
    final_weighted = weighted * factor + pos * own_weight
    lse = highest + jnp.log(final_total)
    loss = lse - pos
    terms = final_weighted / final_total - pos
    temp_grad = (jnp.sum(terms) / total_rows).reshape(1)
    queue_blocks = QUEUE // BLOCK
    targets = ((write_pointer[0] + block_order) % queue_blocks).astype(jnp.int32)
    new_blocks = keys.reshape(total_rows // BLOCK, BLOCK, D)
    new_queue = queue_keys.reshape(queue_blocks, BLOCK, D).at[targets].set(new_blocks).reshape(QUEUE, D)
    return loss, temp_grad, new_queue
```

```python
import functools

import jax
import jax.numpy as jnp
from jax import lax
from jax.experimental import pallas as pl
from jax.experimental.pallas import tpu as pltpu
from jax.sharding import PartitionSpec as P


BLOCK = 128
TILE = 256
LOG2E = 1.4426950408889634
VMEM = pl.BlockSpec(memory_space=pltpu.VMEM)
SMEM = pl.BlockSpec(memory_space=pltpu.SMEM)
HBM = pl.BlockSpec(memory_space=pltpu.HBM)


def accumulate(log_scale, q, k_ref):
    count, rows = q.shape[0], k_ref.shape[0]
    c = jnp.exp(jnp.full((8, count), log_scale, jnp.float32)) * LOG2E
    m = jnp.full((8, count), -jnp.inf, jnp.float32)
    s = jnp.zeros((8, count), jnp.float32)
    w = jnp.zeros((8, count), jnp.float32)
    for t in range(rows // TILE):
        d = lax.dot_general(
            k_ref[pl.ds(t * TILE, TILE), :], q, (((1,), (1,)), ((), ())), preferred_element_type=jnp.float32
        ).reshape(TILE // 8, 8, count)
        higher = jnp.maximum(m, jnp.max(d, axis=0))
        a = jnp.exp2((m - higher) * c)
        e = jnp.exp2((d - higher[None]) * c[None])
        s = s * a + jnp.sum(e, axis=0)
        w = w * a + jnp.sum(e * d, axis=0)
        m = higher
    top = jnp.max(m, axis=0, keepdims=True)
    a = jnp.exp2((m - top) * c)
    return top, jnp.sum(s * a, axis=0, keepdims=True), jnp.sum(w * a, axis=0, keepdims=True)


def first_kernel(ls_ref, qa_ref, qb_ref, k_ref, o_ref, base_ref, sem):
    copy = pltpu.make_async_copy(k_ref, base_ref, sem)
    copy.start()
    for i, row in enumerate(accumulate(ls_ref[0], jnp.concatenate([qa_ref[...], qb_ref[...]], axis=0), k_ref)):
        o_ref[i : i + 1, :] = row
    copy.wait()


def middle_kernel(ls_ref, qa_ref, qb_ref, k_ref, o_ref):
    for i, row in enumerate(accumulate(ls_ref[0], jnp.concatenate([qa_ref[...], qb_ref[...]], axis=0), k_ref)):
        o_ref[i : i + 1, :] = row


def last_kernel(ls_ref, qa_ref, qb_ref, k_ref, pos_ref, *refs):
    *parts, o_ref = refs
    n, tok = o_ref.shape[0], o_ref.shape[2]
    me = lax.axis_index("queue")
    rows = accumulate(ls_ref[0], jnp.concatenate([qa_ref[...], qb_ref[...]], axis=0), k_ref)
    for k in range(n):
        at = jnp.bitwise_xor(me, k)
        for i in range(3):
            lanes = pl.ds((k % 2) * tok, tok)
            row = rows[i][:, (k % 2) * tok : (k % 2 + 1) * tok] if k // 2 == n // 2 - 1 else parts[k // 2][i : i + 1, lanes]
            o_ref[:, pl.ds(i * n + at, 1), :] = jnp.broadcast_to(row[None], (n, 1, tok))
    o_ref[:, 3 * n : 3 * n + 1, :] = jnp.broadcast_to(pos_ref[...][None], (n, 1, tok))


def final_kernel(ls_ref, back_ref, loss_ref, term_ref, hold_ref):
    n, tok = back_ref.shape[0], back_ref.shape[2]
    scale = jnp.exp(jnp.full((n, tok), ls_ref[0], jnp.float32))
    pos = scale * back_ref[:, 3 * n, :]
    peak = back_ref[0, 0:n, :]
    for i in range(1, n):
        peak = jnp.maximum(peak, back_ref[i, 0:n, :])
    total = jnp.zeros((n, tok), jnp.float32)
    weighted = jnp.zeros((n, tok), jnp.float32)
    for i in range(n):
        factor = jnp.exp(scale * (back_ref[i, 0:n, :] - peak))
        total += back_ref[i, n : 2 * n, :] * factor
        weighted += back_ref[i, 2 * n : 3 * n, :] * factor
    peak = scale * peak
    highest = jnp.maximum(peak, pos)
    factor = jnp.exp(peak - highest)
    own = jnp.exp(pos - highest)
    final_total = total * factor + own
    final_weighted = scale * weighted * factor + pos * own
    hold_ref[...] = highest + jnp.log(final_total) - pos
    loss_ref[...] = hold_ref[pl.ds(lax.axis_index("queue"), 1), :]
    terms = final_weighted / final_total - pos
    term_ref[...] = jnp.broadcast_to(jnp.sum(terms, keepdims=True), term_ref.shape)


def enqueue_kernel(n_queue, n_batch, ptr_ref, order_ref, base_ref, *refs):
    *pieces, out_ref, sem = refs
    per_dev = out_ref.shape[0] // BLOCK
    total = per_dev * n_queue
    me_q, me_b = lax.axis_index("queue"), lax.axis_index("batch")
    each = order_ref.shape[0] // (n_queue * n_batch)

    def rows(i):
        return pl.ds(pl.multiple_of(i * BLOCK, BLOCK), BLOCK)

    def slot_of(c):
        at = ptr_ref[0] + order_ref[c]
        at = jnp.where(at >= total, at - total, at) - me_q * per_dev
        return at, (at >= 0) & (at < per_dev)

    def start(c, _):
        slot, mine = slot_of(c)

        @pl.when(mine)
        def _():
            dev, rest = c // each, c % each
            dq, db = jnp.bitwise_xor(dev // n_batch, me_q), jnp.bitwise_xor(dev % n_batch, me_b)
            at = ((dq // 2) * (n_batch // 2) + db // 2) * each + rest
            for j, piece in enumerate(pieces):
                @pl.when(dq % 2 + 2 * (db % 2) == j)
                def _():
                    pltpu.make_async_copy(piece.at[rows(at)], out_ref.at[rows(slot)], sem.at[slot]).start()

        return 0

    def finish(c, _):
        slot, mine = slot_of(c)

        @pl.when(mine)
        def _():
            pltpu.make_async_copy(pieces[0].at[rows(0)], out_ref.at[rows(slot)], sem.at[slot]).wait()

        return 0

    lax.fori_loop(0, order_ref.shape[0], start, 0)
    lax.fori_loop(0, order_ref.shape[0], finish, 0)


def kernel_call(kernel, operands, specs, shapes, out_specs, scratch=(), cost=None, **more):
    return pl.pallas_call(
        kernel,
        out_shape=shapes,
        in_specs=specs,
        out_specs=out_specs,
        scratch_shapes=list(scratch),
        compiler_params=pltpu.CompilerParams(vmem_limit_bytes=12 << 20),
        cost_estimate=cost,
        **more,
    )(*operands)


def per_device(n_queue, n_batch, queries, keys, queue_keys, log_scale, write_pointer, block_order, pos_index):
    tok_rows, width = queries.shape

    def hop(x, axis, n, k):
        return lax.ppermute(x, axis, [(i, i ^ k) for i in range(n)])

    def across(x, k):
        return hop(x, "queue", n_queue, k)

    def beside(x, k):
        return hop(x, "batch", n_batch, k)

    got = [None] * n_queue
    got[0] = queries
    for k in range(2, n_queue, 2):
        got[k] = across(queries, k)
    got[1] = across(queries, 1)
    for k in range(3, n_queue, 2):
        got[k] = across(got[k - 1], 1)

    half = [keys]
    step = n_batch // 2
    while step > 1:
        half = half + [beside(x, step) for x in half]
        step //= 2
    order = [0]
    step = n_batch // 2
    while step > 1:
        order = order + [o ^ step for o in order]
        step //= 2
    half = jnp.concatenate([half[order.index(2 * j)] for j in range(n_batch // 2)], axis=0)
    even = jnp.concatenate([half] + [across(half, k) for k in range(2, n_queue, 2)], axis=0)
    odd = across(even, 1)
    pieces = (even, odd, beside(even, 1), beside(odd, 1))

    local_scores = lax.dot_general(keys, queries, (((1,), (1,)), ((), ())), preferred_element_type=jnp.float32)
    rows = lax.broadcasted_iota(jnp.int32, local_scores.shape, 0)
    pos = jnp.sum(jnp.where(rows == pos_index[None, :], local_scores, 0.0), axis=0, keepdims=True)

    cost = pl.CostEstimate(
        flops=4 * tok_rows * queue_keys.shape[0] * width,
        bytes_accessed=queue_keys.size * 2,
        transcendentals=2 * tok_rows * queue_keys.shape[0],
    )
    part_shape = jax.ShapeDtypeStruct((3, 2 * tok_rows), jnp.float32)
    first, base = kernel_call(
        first_kernel,
        (log_scale, got[0], got[1], queue_keys),
        [SMEM, VMEM, VMEM, VMEM],
        (part_shape, jax.ShapeDtypeStruct(queue_keys.shape, queue_keys.dtype)),
        (VMEM, HBM),
        [pltpu.SemaphoreType.DMA],
        cost,
    )
    parts = [first]
    for k in range(2, n_queue - 2, 2):
        parts.append(
            kernel_call(
                middle_kernel,
                (log_scale, got[k], got[k + 1], queue_keys),
                [SMEM, VMEM, VMEM, VMEM],
                part_shape,
                VMEM,
                cost=cost,
            )
        )
    sent = kernel_call(
        last_kernel,
        (log_scale, got[n_queue - 2], got[n_queue - 1], queue_keys, pos, *parts),
        [SMEM, VMEM, VMEM, VMEM, VMEM] + [VMEM] * len(parts),
        jax.ShapeDtypeStruct((n_queue, 3 * n_queue + 8, tok_rows), jnp.float32),
        VMEM,
        cost=cost,
    )
    back = lax.all_to_all(sent, "queue", split_axis=0, concat_axis=0, tiled=True)
    loss, term = kernel_call(
        final_kernel,
        (log_scale, back),
        [SMEM, VMEM],
        (jax.ShapeDtypeStruct((1, tok_rows), jnp.float32), jax.ShapeDtypeStruct((1, 128), jnp.float32)),
        (VMEM, VMEM),
        [pltpu.VMEM((n_queue, tok_rows), jnp.float32)],
    )
    step = n_batch // 2
    while step:
        term = term + beside(term, step)
        step //= 2
    temp_grad = term[0, :1] / (tok_rows * n_queue * n_batch)

    new_queue = kernel_call(
        functools.partial(enqueue_kernel, n_queue, n_batch),
        (write_pointer, block_order, base, *pieces),
        [SMEM, SMEM, HBM] + [VMEM] * len(pieces),
        jax.ShapeDtypeStruct(queue_keys.shape, queue_keys.dtype),
        HBM,
        [pltpu.SemaphoreType.DMA((queue_keys.shape[0] // BLOCK,))],
        input_output_aliases={2: 0},
    )
    return (loss.reshape(tok_rows), temp_grad, new_queue)


def solution(mesh):
    n_queue, n_batch = mesh.shape["queue"], mesh.shape["batch"]
    placed = (
        P(("queue", "batch"), None),
        P(("queue", "batch"), None),
        P("queue", None),
        P(),
        P(),
        P(),
        P(("queue", "batch")),
    )
    return jax.shard_map(
        functools.partial(per_device, n_queue, n_batch),
        mesh=mesh,
        in_specs=placed,
        out_specs=(P(("queue", "batch")), P(), P("queue", None)),
        check_vma=False,
    )
```

```python
import functools

import jax
import jax.numpy as jnp
from jax import lax
from jax.experimental import pallas as pl
from jax.experimental.pallas import tpu as pltpu
from jax.sharding import PartitionSpec as P


BLOCK = 128
TILE = 256
LOG2E = 1.4426950408889634
LARGE = 2.0**60
VMEM = pl.BlockSpec(memory_space=pltpu.VMEM)
HBM = pl.BlockSpec(memory_space=pltpu.HBM)
SMEM = pl.BlockSpec(memory_space=pltpu.SMEM)


def dot_t(a, b):
    return lax.dot_general(a, b, (((1,), (1,)), ((), ())), preferred_element_type=jnp.float32)


def scores_of(k_ref, q, t):
    return dot_t(k_ref[pl.ds(t * TILE, TILE), :], q).reshape(TILE // 8, 8, q.shape[0])


def settle(m, s, w, c, o_ref):
    top = jnp.max(m, axis=0, keepdims=True)
    a = jnp.exp2((m - top) * c)
    o_ref[0:1, :] = top
    o_ref[1:2, :] = jnp.sum(s * a, axis=0, keepdims=True)
    o_ref[2:3, :] = jnp.sum(w * a, axis=0, keepdims=True)


def accumulate(log_scale, q, k_ref, o_ref):
    count, tiles = q.shape[0], k_ref.shape[0] // TILE
    c = jnp.exp(jnp.broadcast_to(log_scale, (8, count))) * LOG2E
    d = scores_of(k_ref, q, 0)
    m = jnp.max(d, axis=0)
    e = jnp.exp2((d - m[None]) * c[None])
    s = jnp.sum(e, axis=0)
    w = jnp.sum(e * d, axis=0)
    for t in range(1, tiles):
        d = scores_of(k_ref, q, t)
        e = jnp.exp2((d - m[None]) * c[None])
        s = s + jnp.sum(e, axis=0)
        w = w + jnp.sum(e * d, axis=0)
    settle(m, s, w, c, o_ref)

    @pl.when(jnp.logical_not(jnp.max(s) < LARGE))
    def _():
        def step(t, carry):
            m, s, w = carry
            d = scores_of(k_ref, q, t)
            higher = jnp.maximum(m, jnp.max(d, axis=0))
            a = jnp.exp2((m - higher) * c)
            e = jnp.exp2((d - higher[None]) * c[None])
            return higher, s * a + jnp.sum(e, axis=0), w * a + jnp.sum(e * d, axis=0)

        zero = jnp.zeros((8, count), jnp.float32)
        settle(*lax.fori_loop(0, tiles, step, (m, zero, zero)), c, o_ref)


def both(a_ref, b_ref, tok):
    return jnp.concatenate([a_ref[:tok, :], b_ref[:tok, :]], axis=0)


def open_kernel(o_ref):
    o_ref[...] = jnp.zeros_like(o_ref)


def first_kernel(_, ls_ref, index_ref, qa_ref, qb_ref, k_ref, o_ref, pos_ref):
    tok = qa_ref.shape[0] // 2
    scores = dot_t(qa_ref[tok:, :], qa_ref[:tok, :])
    rows = lax.broadcasted_iota(jnp.int32, scores.shape, 0)
    pos_ref[...] = jnp.sum(jnp.where(rows == index_ref[...], scores, 0.0), axis=0, keepdims=True)
    accumulate(ls_ref[...], both(qa_ref, qb_ref, tok), k_ref, o_ref)


def middle_kernel(ls_ref, qa_ref, qb_ref, k_ref, o_ref):
    accumulate(ls_ref[...], both(qa_ref, qb_ref, o_ref.shape[1] // 2), k_ref, o_ref)


def last_kernel(ls_ref, qa_ref, qb_ref, k_ref, pos_ref, *refs):
    *parts, o_ref, hold, own = refs
    n, tok = o_ref.shape[0], o_ref.shape[2]
    me = lax.axis_index("queue")
    hold[3 * n : 3 * n + 1, :] = pos_ref[...]
    for k in range(n - 2):
        at = jnp.bitwise_xor(me, k)
        for i in range(3):
            hold[pl.ds(i * n + at, 1), :] = parts[k // 2][i : i + 1, (k % 2) * tok : (k % 2 + 1) * tok]
    accumulate(ls_ref[...], both(qa_ref, qb_ref, tok), k_ref, own)
    for k in range(n - 2, n):
        at = jnp.bitwise_xor(me, k)
        for i in range(3):
            hold[pl.ds(i * n + at, 1), :] = own[i : i + 1, (k % 2) * tok : (k % 2 + 1) * tok]
    sent = hold[...]
    for i in range(n):
        o_ref[i] = sent


def base_kernel(_, ptr_ref, order_ref, k_ref, base_ref, sem):
    copy = pltpu.make_async_copy(k_ref, base_ref, sem)
    copy.start()
    copy.wait()


def final_kernel(ls_ref, back_ref, loss_ref, term_ref, hold_ref):
    n, tok = back_ref.shape[0], back_ref.shape[2]
    scale = jnp.exp(jnp.broadcast_to(ls_ref[...], (n, tok)))
    pos = scale * back_ref[:, 3 * n, :]
    peak = back_ref[0, 0:n, :]
    for i in range(1, n):
        peak = jnp.maximum(peak, back_ref[i, 0:n, :])
    total = jnp.zeros((n, tok), jnp.float32)
    weighted = jnp.zeros((n, tok), jnp.float32)
    for i in range(n):
        factor = jnp.exp(scale * (back_ref[i, 0:n, :] - peak))
        total += back_ref[i, n : 2 * n, :] * factor
        weighted += back_ref[i, 2 * n : 3 * n, :] * factor
    peak = scale * peak
    highest = jnp.maximum(peak, pos)
    factor = jnp.exp(peak - highest)
    own = jnp.exp(pos - highest)
    final_total = total * factor + own
    final_weighted = scale * weighted * factor + pos * own
    hold_ref[...] = highest + jnp.log(final_total) - pos
    loss_ref[...] = hold_ref[pl.ds(lax.axis_index("queue"), 1), :]
    terms = final_weighted / final_total - pos
    mean = jnp.sum(terms, keepdims=True) / (n * tok * lax.axis_size("batch"))
    term_ref[...] = jnp.broadcast_to(mean, term_ref.shape)


def grad_kernel(*refs):
    *terms, o_ref = refs
    o_ref[...] = sum((x[0:1, 0:1] for x in terms[1:]), terms[0][0:1, 0:1])


def enqueue_kernel(n_queue, n_batch, order, ptr, block_order, base_ref, *refs):
    *pieces, out_ref, sem = refs
    per_dev = out_ref.shape[0] // BLOCK
    total = per_dev * n_queue
    count = block_order.shape[0]
    each = count // (n_queue * n_batch)
    me_q, me_b = lax.axis_index("queue"), lax.axis_index("batch")
    offset = ptr[0] - me_q * per_dev
    offset = jnp.where(offset < 0, offset + total, offset)

    def rows(i):
        return pl.ds(pl.multiple_of(i * BLOCK, BLOCK), BLOCK)

    def slot_of(c):
        at = offset + block_order[c]
        return jnp.where(at >= total, at - total, at)

    def start(c, _):
        slot = slot_of(c)

        @pl.when(slot < per_dev)
        def _():
            dev = c // each
            dq, db = jnp.bitwise_xor(dev // n_batch, me_q), jnp.bitwise_xor(dev % n_batch, me_b)
            at = jnp.where(dq < 4, dq, dq - 4) * each + c % each
            for (b, p), piece in zip(order, pieces):
                @pl.when((db == b) & (dq >= 4 if p else dq < 4))
                def _():
                    pltpu.make_async_copy(piece.at[rows(at)], out_ref.at[rows(slot)], sem.at[slot]).start()

        return 0

    def finish(c, _):
        slot = slot_of(c)

        @pl.when(slot < per_dev)
        def _():
            pltpu.make_async_copy(pieces[0].at[rows(0)], out_ref.at[rows(slot)], sem.at[slot]).wait()

        return 0

    @pl.when((offset < per_dev) | (offset + count > total))
    def _():
        lax.fori_loop(0, count, start, 0, unroll=4)
        lax.fori_loop(0, count, finish, 0, unroll=4)


def kernel_call(kernel, operands, specs, shapes, out_specs, scratch=(), cost=None, **more):
    return pl.pallas_call(
        kernel,
        out_shape=shapes,
        in_specs=specs,
        out_specs=out_specs,
        scratch_shapes=list(scratch),
        compiler_params=pltpu.CompilerParams(vmem_limit_bytes=12 << 20),
        cost_estimate=cost,
        **more,
    )(*operands)


def evens(n):
    return sorted(range(2, n, 2), key=lambda k: (bin(k).count("1"), -k))


def per_device(n_queue, n_batch, queries, keys, queue_keys, log_scale, write_pointer, block_order, pos_index):
    tok, width = queries.shape

    def hop(x, axis, n, k):
        return lax.ppermute(x, axis, [(i, i ^ k) for i in range(n)])

    def across(x, k):
        return hop(x, "queue", n_queue, k)

    def beside(x, k):
        return hop(x, "batch", n_batch, k)

    cost = pl.CostEstimate(
        flops=4 * tok * queue_keys.shape[0] * width,
        bytes_accessed=queue_keys.size * 2,
        transcendentals=2 * tok * queue_keys.shape[0],
    )
    ls = log_scale.reshape(1, 1)
    opened = kernel_call(open_kernel, (), [], jax.ShapeDtypeStruct((8, 128), jnp.float32), VMEM, cost=cost)

    got = [None] * n_queue
    far = [k for k in evens(n_queue) if k > 2]
    for k in far:
        low = k & -k
        got[k] = across(got[k - low] if k > low else queries, low)
    above = lax.broadcasted_iota(jnp.int32, (2 * tok, width), 0) < tok
    got[0] = jnp.where(above, jnp.pad(queries, ((0, tok), (0, 0))), jnp.pad(keys, ((tok, 0), (0, 0))))
    for k in (2, 1, 3):
        if k < n_queue:
            got[k] = across(got[k - 1] if k == 3 else got[0], 2 if k == 2 else 1)
    far_keys = {}
    for k in far:
        low = k & -k
        far_keys[k] = across(far_keys[k - low] if k > low else keys, low)
        got[k + 1] = across(jnp.concatenate([got[k], far_keys[k]], axis=0), 1)
        far_keys[k + 1] = got[k + 1][tok:]

    pieces = {(0, 0): jnp.concatenate([x[tok:] for x in got[:4]], axis=0)}
    if far:
        pieces[0, 1] = jnp.concatenate([far_keys[k] for k in sorted(far_keys)], axis=0)
    step = n_batch // 2
    while step:
        for (b, p), x in list(pieces.items()):
            pieces[b ^ step, p] = beside(x, step)
        step //= 2
    order = list(pieces)

    part_shape = jax.ShapeDtypeStruct((3, 2 * tok), jnp.float32)
    queue_shape = jax.ShapeDtypeStruct(queue_keys.shape, queue_keys.dtype)
    first, pos = kernel_call(
        first_kernel,
        (opened, ls, pos_index.reshape(1, tok), got[0], got[1], queue_keys),
        [VMEM] * 6,
        (part_shape, jax.ShapeDtypeStruct((1, tok), jnp.float32)),
        (VMEM, VMEM),
        cost=cost,
    )
    parts = [first]
    for k in range(2, n_queue - 2, 2):
        parts.append(
            kernel_call(
                middle_kernel, (ls, got[k], got[k + 1], queue_keys), [VMEM] + [VMEM] * 3, part_shape, VMEM, cost=cost
            )
        )
    sent = kernel_call(
        last_kernel,
        (ls, got[n_queue - 2], got[n_queue - 1], queue_keys, pos, *parts),
        [VMEM] + [VMEM] * (4 + len(parts)),
        jax.ShapeDtypeStruct((n_queue, 3 * n_queue + 8, tok), jnp.float32),
        VMEM,
        [
            pltpu.VMEM((3 * n_queue + 8, tok), jnp.float32),
            pltpu.VMEM((3, 2 * tok), jnp.float32),
        ],
        cost=cost,
    )
    base = kernel_call(
        base_kernel, (first, write_pointer, block_order, queue_keys), [HBM, SMEM, SMEM, VMEM], queue_shape, HBM, [pltpu.SemaphoreType.DMA], cost=cost
    )
    back = lax.all_to_all(sent, "queue", split_axis=0, concat_axis=0, tiled=True)
    loss, term = kernel_call(
        final_kernel,
        (ls, back),
        [VMEM, VMEM],
        (jax.ShapeDtypeStruct((1, tok), jnp.float32), jax.ShapeDtypeStruct((1, tok), jnp.float32)),
        (VMEM, VMEM),
        [pltpu.VMEM((n_queue, tok), jnp.float32)],
    )
    terms = [term] + [beside(term, k) for k in range(n_batch - 1, 0, -1)]
    temp_grad = kernel_call(grad_kernel, terms, [VMEM] * n_batch, jax.ShapeDtypeStruct((1, 1), jnp.float32), VMEM)
    new_queue = kernel_call(
        functools.partial(enqueue_kernel, n_queue, n_batch, order),
        (write_pointer, block_order, base, *pieces.values()),
        [SMEM, SMEM, HBM] + [VMEM] * len(pieces),
        queue_shape,
        HBM,
        [pltpu.SemaphoreType.DMA((queue_keys.shape[0] // BLOCK,))],
        input_output_aliases={2: 0},
    )
    return (loss.reshape(tok), temp_grad.reshape(1), new_queue)


def solution(mesh):
    n_queue, n_batch = mesh.shape["queue"], mesh.shape["batch"]
    placed = (
        P(("queue", "batch"), None),
        P(("queue", "batch"), None),
        P("queue", None),
        P(),
        P(),
        P(),
        P(("queue", "batch")),
    )
    return jax.shard_map(
        functools.partial(per_device, n_queue, n_batch),
        mesh=mesh,
        in_specs=placed,
        out_specs=(P(("queue", "batch")), P(), P("queue", None)),
        check_vma=False,
    )
```

```python
import functools

import jax
import jax.numpy as jnp
from jax import lax
from jax.experimental import pallas as pl
from jax.experimental.pallas import tpu as pltpu
from jax.sharding import PartitionSpec as P


BLOCK = 128
TILE = 256
LOG2E = 1.4426950408889634
LARGE = 2.0**60
VMEM = pl.BlockSpec(memory_space=pltpu.VMEM)
HBM = pl.BlockSpec(memory_space=pltpu.HBM)
SMEM = pl.BlockSpec(memory_space=pltpu.SMEM)


def dot_t(a, b):
    return lax.dot_general(a, b, (((1,), (1,)), ((), ())), preferred_element_type=jnp.float32)


def scores_of(k_ref, q, t):
    return dot_t(k_ref[pl.ds(t * TILE, TILE), :], q).reshape(TILE // 8, 8, q.shape[0])


def settle(m, s, w, c, o_ref):
    top = jnp.max(m, axis=0, keepdims=True)
    a = jnp.exp2((m - top) * c)
    o_ref[0:1, :] = top
    o_ref[1:2, :] = jnp.sum(s * a, axis=0, keepdims=True)
    o_ref[2:3, :] = jnp.sum(w * a, axis=0, keepdims=True)


def accumulate(rate_ref, q, k_ref, o_ref):
    count, tiles = q.shape[0], k_ref.shape[0] // TILE
    c = jnp.concatenate([rate_ref[...]] * (count // rate_ref.shape[1]), axis=1) * LOG2E
    d = scores_of(k_ref, q, 0)
    m = jnp.max(d, axis=0)
    e = jnp.exp2((d - m[None]) * c[None])
    s = jnp.sum(e, axis=0)
    w = jnp.sum(e * d, axis=0)
    for t in range(1, tiles):
        d = scores_of(k_ref, q, t)
        e = jnp.exp2((d - m[None]) * c[None])
        s = s + jnp.sum(e, axis=0)
        w = w + jnp.sum(e * d, axis=0)
    settle(m, s, w, c, o_ref)

    @pl.when(jnp.logical_not(jnp.max(s) < LARGE))
    def _():
        def step(t, carry):
            m, s, w = carry
            d = scores_of(k_ref, q, t)
            higher = jnp.maximum(m, jnp.max(d, axis=0))
            a = jnp.exp2((m - higher) * c)
            e = jnp.exp2((d - higher[None]) * c[None])
            return higher, s * a + jnp.sum(e, axis=0), w * a + jnp.sum(e * d, axis=0)

        zero = jnp.zeros((8, count), jnp.float32)
        settle(*lax.fori_loop(0, tiles, step, (m, zero, zero)), c, o_ref)


def both(a_ref, b_ref, tok):
    return jnp.concatenate([a_ref[:tok, :], b_ref[:tok, :]], axis=0)


def open_kernel(o_ref):
    o_ref[...] = jnp.zeros_like(o_ref)


def first_kernel(_, rate_ref, index_ref, qa_ref, qb_ref, k_ref, o_ref, pos_ref):
    tok = qa_ref.shape[0] // 2
    scores = dot_t(qa_ref[tok:, :], qa_ref[:tok, :])
    rows = lax.broadcasted_iota(jnp.int32, scores.shape, 0)
    pos_ref[...] = jnp.sum(jnp.where(rows == index_ref[...], scores, 0.0), axis=0, keepdims=True)
    accumulate(rate_ref, both(qa_ref, qb_ref, tok), k_ref, o_ref)


def middle_kernel(rate_ref, qa_ref, qb_ref, k_ref, o_ref):
    accumulate(rate_ref, both(qa_ref, qb_ref, o_ref.shape[1] // 2), k_ref, o_ref)


def last_kernel(rate_ref, qa_ref, qb_ref, k_ref, pos_ref, *refs):
    *parts, o_ref, hold, own = refs
    n, tok = o_ref.shape[0], o_ref.shape[2]
    me = lax.axis_index("queue")
    hold[3 * n : 3 * n + 1, :] = pos_ref[...]
    for k in range(n - 2):
        at = jnp.bitwise_xor(me, k)
        for i in range(3):
            hold[pl.ds(i * n + at, 1), :] = parts[k // 2][i : i + 1, (k % 2) * tok : (k % 2 + 1) * tok]
    accumulate(rate_ref, both(qa_ref, qb_ref, tok), k_ref, own)
    for k in range(n - 2, n):
        at = jnp.bitwise_xor(me, k)
        for i in range(3):
            hold[pl.ds(i * n + at, 1), :] = own[i : i + 1, (k % 2) * tok : (k % 2 + 1) * tok]
    sent = hold[...]
    for i in range(n):
        o_ref[i] = sent


def places(n_queue, n_batch, split, order, ptr, block_order, per_dev):
    total = per_dev * n_queue
    count = block_order.shape[0]
    each = count // (n_queue * n_batch)
    me_q, me_b = lax.axis_index("queue"), lax.axis_index("batch")
    offset = ptr[0] - me_q * per_dev
    offset = jnp.where(offset < 0, offset + total, offset)

    def slot_of(c):
        at = offset + block_order[c]
        return jnp.where(at >= total, at - total, at)

    def from_piece(c, pieces, group, use):
        dev = c // each
        dq, db = jnp.bitwise_xor(dev // n_batch, me_q), jnp.bitwise_xor(dev % n_batch, me_b)
        at = (dq - split if group else dq) * each + c % each
        for b, piece in zip(order, pieces):
            @pl.when((db == b) & ((dq >= split) if group else (dq < split)))
            def _():
                use(piece.at[rows_of(at)])

    return (offset < per_dev) | (offset + count > total), slot_of, from_piece


def rows_of(i):
    return pl.ds(pl.multiple_of(i * BLOCK, BLOCK), BLOCK)


def base_kernel(n_queue, n_batch, split, order, _, ptr, block_order, k_ref, *refs):
    *pieces, out_ref, table, sem, whole = refs
    per_dev = out_ref.shape[0] // BLOCK
    count = block_order.shape[0]
    hit, slot_of, from_piece = places(n_queue, n_batch, split, order, ptr, block_order, per_dev)

    @pl.when(jnp.logical_not(hit))
    def _():
        copy = pltpu.make_async_copy(k_ref, out_ref, whole)
        copy.start()
        copy.wait()

    def clear(s, _):
        table[s] = -1
        return 0

    def fill(c, _):
        slot = slot_of(c)

        @pl.when(slot < per_dev)
        def _():
            table[slot] = c

        return 0

    def mine(s):
        dq = jnp.bitwise_xor(table[s] // (count // n_queue), lax.axis_index("queue"))
        return (table[s] < 0) | (dq < split)

    def start(s, _):
        def put(source):
            pltpu.make_async_copy(source, out_ref.at[rows_of(s)], sem.at[s]).start()

        @pl.when(table[s] < 0)
        def _():
            put(k_ref.at[rows_of(s)])

        @pl.when(table[s] >= 0)
        def _():
            from_piece(table[s], pieces, 0, put)

        return 0

    def finish(s, _):
        @pl.when(mine(s))
        def _():
            pltpu.make_async_copy(k_ref.at[rows_of(s)], out_ref.at[rows_of(s)], sem.at[s]).wait()

        return 0

    @pl.when(hit)
    def _():
        lax.fori_loop(0, per_dev, clear, 0)
        lax.fori_loop(0, count, fill, 0)
        lax.fori_loop(0, per_dev, start, 0)
        lax.fori_loop(0, per_dev, finish, 0)


def final_kernel(rate_ref, back_ref, loss_ref, term_ref, hold_ref):
    n, tok = back_ref.shape[0], back_ref.shape[2]
    scale = jnp.broadcast_to(rate_ref[0:1, :], (n, tok))
    pos = scale * back_ref[:, 3 * n, :]
    peak = back_ref[0, 0:n, :]
    for i in range(1, n):
        peak = jnp.maximum(peak, back_ref[i, 0:n, :])
    total = jnp.zeros((n, tok), jnp.float32)
    weighted = jnp.zeros((n, tok), jnp.float32)
    for i in range(n):
        factor = jnp.exp(scale * (back_ref[i, 0:n, :] - peak))
        total += back_ref[i, n : 2 * n, :] * factor
        weighted += back_ref[i, 2 * n : 3 * n, :] * factor
    peak = scale * peak
    highest = jnp.maximum(peak, pos)
    factor = jnp.exp(peak - highest)
    own = jnp.exp(pos - highest)
    final_total = total * factor + own
    final_weighted = scale * weighted * factor + pos * own
    hold_ref[...] = highest + jnp.log(final_total) - pos
    loss_ref[...] = hold_ref[pl.ds(lax.axis_index("queue"), 1), :]
    terms = final_weighted / final_total - pos
    mean = jnp.sum(terms, keepdims=True) / (n * tok * lax.axis_size("batch"))
    term_ref[...] = jnp.broadcast_to(mean, term_ref.shape)


def grad_kernel(*refs):
    *terms, o_ref = refs
    o_ref[...] = sum((x[0:1, 0:1] for x in terms[1:]), terms[0][0:1, 0:1])


def enqueue_kernel(n_queue, n_batch, split, order, ptr, block_order, base_ref, *refs):
    *pieces, out_ref, sem = refs
    per_dev = out_ref.shape[0] // BLOCK
    count = block_order.shape[0]
    hit, slot_of, from_piece = places(n_queue, n_batch, split, order, ptr, block_order, per_dev)

    def ours(c):
        dq = jnp.bitwise_xor(c // (count // n_queue), lax.axis_index("queue"))
        slot = slot_of(c)
        return slot, (slot < per_dev) & (dq >= split)

    def start(c, _):
        slot, write = ours(c)

        @pl.when(write)
        def _():
            from_piece(
                c, pieces, 1, lambda x: pltpu.make_async_copy(x, out_ref.at[rows_of(slot)], sem.at[slot]).start()
            )

        return 0

    def finish(c, _):
        slot, write = ours(c)

        @pl.when(write)
        def _():
            pltpu.make_async_copy(pieces[0].at[rows_of(0)], out_ref.at[rows_of(slot)], sem.at[slot]).wait()

        return 0

    @pl.when(hit)
    def _():
        lax.fori_loop(0, count, start, 0)
        lax.fori_loop(0, count, finish, 0)


def kernel_call(kernel, operands, specs, shapes, out_specs, scratch=(), cost=None, **more):
    return pl.pallas_call(
        kernel,
        out_shape=shapes,
        in_specs=specs,
        out_specs=out_specs,
        scratch_shapes=list(scratch),
        compiler_params=pltpu.CompilerParams(vmem_limit_bytes=12 << 20),
        cost_estimate=cost,
        **more,
    )(*operands)


def evens(n):
    return sorted(range(2, n, 2), key=lambda k: (bin(k).count("1"), -k))


def per_device(n_queue, n_batch, queries, keys, queue_keys, log_scale, write_pointer, block_order, pos_index):
    tok, width = queries.shape

    def hop(x, axis, n, k):
        return lax.ppermute(x, axis, [(i, i ^ k) for i in range(n)])

    def across(x, k):
        return hop(x, "queue", n_queue, k)

    def beside(x, k):
        return hop(x, "batch", n_batch, k)

    cost = pl.CostEstimate(
        flops=4 * tok * queue_keys.shape[0] * width,
        bytes_accessed=queue_keys.size * 2,
        transcendentals=2 * tok * queue_keys.shape[0],
    )
    rate = jnp.broadcast_to(jnp.exp(log_scale), (8, tok))
    wait = pl.CostEstimate(flops=64 * cost.flops, bytes_accessed=4096, transcendentals=0)
    opened = kernel_call(open_kernel, (), [], jax.ShapeDtypeStruct((8, 128), jnp.float32), VMEM, cost=wait)

    got = [None] * n_queue
    far = [k for k in evens(n_queue) if k > 2]
    for k in far:
        low = k & -k
        got[k] = across(got[k - low] if k > low else queries, low)
    above = lax.broadcasted_iota(jnp.int32, (2 * tok, width), 0) < tok
    got[0] = jnp.where(above, jnp.pad(queries, ((0, tok), (0, 0))), jnp.pad(keys, ((tok, 0), (0, 0))))
    for k in (2, 1, 3):
        if k < n_queue:
            got[k] = across(got[k - 1] if k == 3 else got[0], 2 if k == 2 else 1)
    far_keys = {}
    for k in far:
        low = k & -k
        far_keys[k] = across(far_keys[k - low] if k > low else keys, low)
        got[k + 1] = across(jnp.concatenate([got[k], far_keys[k]], axis=0), 1)
        far_keys[k + 1] = got[k + 1][tok:]

    far_keys.update((k, x[tok:]) for k, x in enumerate(got[:4]))
    split = max(5 * n_queue // 8, 1)
    pieces = {(0, 0): jnp.concatenate([far_keys[k] for k in range(split)], axis=0)}
    pieces[0, 1] = jnp.concatenate([far_keys[k] for k in range(split, n_queue)], axis=0)
    step = n_batch // 2
    while step:
        for (b, p), x in list(pieces.items()):
            pieces[b ^ step, p] = beside(x, step)
        step //= 2

    part_shape = jax.ShapeDtypeStruct((3, 2 * tok), jnp.float32)
    queue_shape = jax.ShapeDtypeStruct(queue_keys.shape, queue_keys.dtype)
    first, pos = kernel_call(
        first_kernel,
        (opened, rate, pos_index.reshape(1, tok), got[0], got[1], queue_keys),
        [VMEM] * 6,
        (part_shape, jax.ShapeDtypeStruct((1, tok), jnp.float32)),
        (VMEM, VMEM),
        cost=cost,
    )
    parts = [first]
    for k in range(2, n_queue - 2, 2):
        parts.append(
            kernel_call(
                middle_kernel, (rate, got[k], got[k + 1], queue_keys), [VMEM] + [VMEM] * 3, part_shape, VMEM, cost=cost
            )
        )
    sent = kernel_call(
        last_kernel,
        (rate, got[n_queue - 2], got[n_queue - 1], queue_keys, pos, *parts),
        [VMEM] + [VMEM] * (4 + len(parts)),
        jax.ShapeDtypeStruct((n_queue, 3 * n_queue + 8, tok), jnp.float32),
        VMEM,
        [
            pltpu.VMEM((3 * n_queue + 8, tok), jnp.float32),
            pltpu.VMEM((3, 2 * tok), jnp.float32),
        ],
        cost=cost,
    )
    order = [b for b, p in pieces if p == 0]
    groups = [[pieces[b, p] for b in order] for p in range(2)]
    where = (n_queue, n_batch, split, order)
    per_dev = queue_keys.shape[0] // BLOCK
    base = kernel_call(
        functools.partial(base_kernel, *where),
        (first, write_pointer, block_order, queue_keys, *groups[0]),
        [HBM, SMEM, SMEM, VMEM] + [VMEM] * n_batch,
        queue_shape,
        HBM,
        [pltpu.SMEM((per_dev,), jnp.int32), pltpu.SemaphoreType.DMA((per_dev,)), pltpu.SemaphoreType.DMA],
        cost=cost,
    )
    back = lax.all_to_all(sent, "queue", split_axis=0, concat_axis=0, tiled=True)
    loss, term = kernel_call(
        final_kernel,
        (rate, back),
        [VMEM, VMEM],
        (jax.ShapeDtypeStruct((1, tok), jnp.float32), jax.ShapeDtypeStruct((1, tok), jnp.float32)),
        (VMEM, VMEM),
        [pltpu.VMEM((n_queue, tok), jnp.float32)],
    )
    terms = [term] + [beside(term, k) for k in range(n_batch - 1, 0, -1)]
    temp_grad = kernel_call(grad_kernel, terms, [VMEM] * n_batch, jax.ShapeDtypeStruct((1, 1), jnp.float32), VMEM)
    new_queue = kernel_call(
        functools.partial(enqueue_kernel, *where),
        (write_pointer, block_order, base, *groups[1]),
        [SMEM, SMEM, HBM] + [VMEM] * n_batch,
        queue_shape,
        HBM,
        [pltpu.SemaphoreType.DMA((per_dev,))],
        input_output_aliases={2: 0},
    )
    return (loss.reshape(tok), temp_grad.reshape(1), new_queue)


def solution(mesh):
    n_queue, n_batch = mesh.shape["queue"], mesh.shape["batch"]
    placed = (
        P(("queue", "batch"), None),
        P(("queue", "batch"), None),
        P("queue", None),
        P(),
        P(),
        P(),
        P(("queue", "batch")),
    )
    return jax.shard_map(
        functools.partial(per_device, n_queue, n_batch),
        mesh=mesh,
        in_specs=placed,
        out_specs=(P(("queue", "batch")), P(), P("queue", None)),
        check_vma=False,
    )
```

```python
import functools

import jax
import jax.numpy as jnp
from jax import lax
from jax.experimental import pallas as pl
from jax.experimental.pallas import tpu as pltpu
from jax.sharding import PartitionSpec as P


BLOCK = 128
TILE = 256
LOG2E = 1.4426950408889634
LARGE = 2.0**60
VMEM = pl.BlockSpec(memory_space=pltpu.VMEM)
HBM = pl.BlockSpec(memory_space=pltpu.HBM)
SMEM = pl.BlockSpec(memory_space=pltpu.SMEM)


def dot_t(a, b):
    return lax.dot_general(a, b, (((1,), (1,)), ((), ())), preferred_element_type=jnp.float32)


def scores_of(k_ref, q, t):
    return dot_t(k_ref[pl.ds(t * TILE, TILE), :], q).reshape(TILE // 8, 8, q.shape[0])


def settle(m, s, w, c, o_ref):
    top = jnp.max(m, axis=0, keepdims=True)
    a = jnp.exp2((m - top) * c)
    o_ref[0:1, :] = top
    o_ref[1:2, :] = jnp.sum(s * a, axis=0, keepdims=True)
    o_ref[2:3, :] = jnp.sum(w * a, axis=0, keepdims=True)


def accumulate(rate_ref, q, k_ref, o_ref):
    count, tiles = q.shape[0], k_ref.shape[0] // TILE
    c = jnp.concatenate([rate_ref[...]] * (count // rate_ref.shape[1]), axis=1) * LOG2E
    d = scores_of(k_ref, q, 0)
    m = jnp.max(d, axis=0)
    e = jnp.exp2((d - m[None]) * c[None])
    s = jnp.sum(e, axis=0)
    w = jnp.sum(e * d, axis=0)
    for t in range(1, tiles):
        d = scores_of(k_ref, q, t)
        e = jnp.exp2((d - m[None]) * c[None])
        s = s + jnp.sum(e, axis=0)
        w = w + jnp.sum(e * d, axis=0)
    settle(m, s, w, c, o_ref)

    @pl.when(jnp.logical_not(jnp.max(s) < LARGE))
    def _():
        def step(t, carry):
            m, s, w = carry
            d = scores_of(k_ref, q, t)
            higher = jnp.maximum(m, jnp.max(d, axis=0))
            a = jnp.exp2((m - higher) * c)
            e = jnp.exp2((d - higher[None]) * c[None])
            return higher, s * a + jnp.sum(e, axis=0), w * a + jnp.sum(e * d, axis=0)

        zero = jnp.zeros((8, count), jnp.float32)
        settle(*lax.fori_loop(0, tiles, step, (m, zero, zero)), c, o_ref)


def both(a_ref, b_ref, tok):
    return jnp.concatenate([a_ref[:tok, :], b_ref[:tok, :]], axis=0)


def open_kernel(o_ref):
    o_ref[...] = jnp.zeros_like(o_ref)


def first_kernel(_, rate_ref, index_ref, qa_ref, qb_ref, k_ref, o_ref, pos_ref):
    tok = qa_ref.shape[0] // 2
    scores = dot_t(qa_ref[tok:, :], qa_ref[:tok, :])
    rows = lax.broadcasted_iota(jnp.int32, scores.shape, 0)
    pos_ref[...] = jnp.sum(jnp.where(rows == index_ref[...], scores, 0.0), axis=0, keepdims=True)
    accumulate(rate_ref, both(qa_ref, qb_ref, tok), k_ref, o_ref)


def middle_kernel(rate_ref, qa_ref, qb_ref, k_ref, o_ref):
    accumulate(rate_ref, both(qa_ref, qb_ref, o_ref.shape[1] // 2), k_ref, o_ref)


def last_kernel(pairs, rate_ref, qa_ref, qb_ref, k_ref, pos_ref, *refs):
    *parts, o_ref, own = refs
    n, tok = o_ref.shape[0] // 4, o_ref.shape[1]
    me = lax.axis_index("queue")
    o_ref[3 * n :, :] = jnp.zeros((n, tok), jnp.float32)
    o_ref[pl.ds(3 * n + me, 1), :] = pos_ref[...]

    def lay(pair, part):
        for j, k in enumerate(pair):
            at = jnp.bitwise_xor(me, k)
            for i in range(3):
                o_ref[pl.ds(i * n + at, 1), :] = part[i : i + 1, j * tok : (j + 1) * tok]

    for pair, part in zip(pairs, parts):
        lay(pair, part)
    accumulate(rate_ref, both(qa_ref, qb_ref, tok), k_ref, own)
    lay(pairs[-1], own)


def merge_kernel(rate_ref, a_ref, b_ref, o_ref):
    n, tok = o_ref.shape[0] // 4, o_ref.shape[1]
    scale = jnp.broadcast_to(rate_ref[0:1, :], (n, tok))
    ours, theirs = a_ref[0:n, :], b_ref[0:n, :]
    level = jnp.maximum(ours, theirs)
    f, g = jnp.exp(scale * (ours - level)), jnp.exp(scale * (theirs - level))
    o_ref[0:n, :] = level
    o_ref[n : 2 * n, :] = a_ref[n : 2 * n, :] * f + b_ref[n : 2 * n, :] * g
    o_ref[2 * n : 3 * n, :] = a_ref[2 * n : 3 * n, :] * f + b_ref[2 * n : 3 * n, :] * g
    o_ref[3 * n :, :] = a_ref[3 * n :, :] + b_ref[3 * n :, :]


def base_kernel(_, k_ref, base_ref, sem):
    copy = pltpu.make_async_copy(k_ref, base_ref, sem)
    copy.start()
    copy.wait()


def final_kernel(rate_ref, stats_ref, loss_ref, term_ref, hold_ref):
    n, tok = stats_ref.shape[0] // 4, stats_ref.shape[1]
    scale = jnp.broadcast_to(rate_ref[0:1, :], (n, tok))
    peak = scale * stats_ref[0:n, :]
    total = stats_ref[n : 2 * n, :]
    weighted = stats_ref[2 * n : 3 * n, :]
    pos = scale * stats_ref[3 * n :, :]
    highest = jnp.maximum(peak, pos)
    factor = jnp.exp(peak - highest)
    own = jnp.exp(pos - highest)
    final_total = total * factor + own
    final_weighted = scale * weighted * factor + pos * own
    hold_ref[...] = highest + jnp.log(final_total) - pos
    loss_ref[...] = hold_ref[pl.ds(lax.axis_index("queue"), 1), :]
    terms = final_weighted / final_total - pos
    mean = jnp.sum(terms, keepdims=True) / (n * tok * lax.axis_size("batch"))
    term_ref[...] = jnp.broadcast_to(mean, term_ref.shape)


def grad_kernel(*refs):
    *terms, o_ref = refs
    o_ref[...] = sum((x[0:1, 0:1] for x in terms[1:]), terms[0][0:1, 0:1])


def enqueue_kernel(n_queue, n_batch, split, held, ptr, block_order, base_ref, *refs):
    *pieces, out_ref, sem = refs
    per_dev = out_ref.shape[0] // BLOCK
    total = per_dev * n_queue
    count = block_order.shape[0]
    each = count // (n_queue * n_batch)
    me_q, me_b = lax.axis_index("queue"), lax.axis_index("batch")
    offset = ptr[0] - me_q * per_dev
    offset = jnp.where(offset < 0, offset + total, offset)

    def rows(i):
        return pl.ds(pl.multiple_of(i * BLOCK, BLOCK), BLOCK)

    def slot_of(c):
        at = offset + block_order[c]
        return jnp.where(at >= total, at - total, at)

    def start(c, _):
        slot = slot_of(c)

        @pl.when(slot < per_dev)
        def _():
            dev = c // each
            dq, db = jnp.bitwise_xor(dev // n_batch, me_q), jnp.bitwise_xor(dev % n_batch, me_b)
            late = dq >= split
            at = jnp.where(late, dq - split, dq) * each + c % each
            for (b, p), piece in zip(held, pieces):
                @pl.when((db == b) & (late if p else jnp.logical_not(late)))
                def _():
                    pltpu.make_async_copy(piece.at[rows(at)], out_ref.at[rows(slot)], sem.at[slot]).start()

        return 0

    def finish(c, _):
        slot = slot_of(c)

        @pl.when(slot < per_dev)
        def _():
            pltpu.make_async_copy(pieces[0].at[rows(0)], out_ref.at[rows(slot)], sem.at[slot]).wait()

        return 0

    @pl.when((offset < per_dev) | (offset + count > total))
    def _():
        lax.fori_loop(0, count, start, 0)
        lax.fori_loop(0, count, finish, 0)


def kernel_call(kernel, operands, specs, shapes, out_specs, scratch=(), cost=None, **more):
    return pl.pallas_call(
        kernel,
        out_shape=shapes,
        in_specs=specs,
        out_specs=out_specs,
        scratch_shapes=list(scratch),
        compiler_params=pltpu.CompilerParams(vmem_limit_bytes=12 << 20),
        cost_estimate=cost,
        **more,
    )(*operands)


def evens(n):
    return sorted(range(2, n, 2), key=lambda k: (bin(k).count("1"), -k))


def pairs_of(n):
    early, late = range(4, n, 2), range(5, n, 2)
    return [(0, 1), *zip(early[::2], early[1::2]), (2, 3), *zip(late[::2], late[1::2])]


def per_device(n_queue, n_batch, queries, keys, queue_keys, log_scale, write_pointer, block_order, pos_index):
    tok, width = queries.shape

    def hop(x, axis, n, k):
        return lax.ppermute(x, axis, [(i, i ^ k) for i in range(n)])

    def across(x, k):
        return hop(x, "queue", n_queue, k)

    def beside(x, k):
        return hop(x, "batch", n_batch, k)

    cost = pl.CostEstimate(
        flops=4 * tok * queue_keys.shape[0] * width,
        bytes_accessed=queue_keys.size * 2,
        transcendentals=2 * tok * queue_keys.shape[0],
    )
    rate = jnp.broadcast_to(jnp.exp(log_scale), (8, tok))
    wait = pl.CostEstimate(flops=64 * cost.flops, bytes_accessed=4096, transcendentals=0)
    opened = kernel_call(open_kernel, (), [], jax.ShapeDtypeStruct((8, 128), jnp.float32), VMEM, cost=wait)

    got = [None] * n_queue
    far = [k for k in evens(n_queue) if k > 2]
    for k in far:
        low = k & -k
        got[k] = across(got[k - low] if k > low else queries, low)
    above = lax.broadcasted_iota(jnp.int32, (2 * tok, width), 0) < tok
    got[0] = jnp.where(above, jnp.pad(queries, ((0, tok), (0, 0))), jnp.pad(keys, ((tok, 0), (0, 0))))
    for k in (2, 1, 3):
        if k < n_queue:
            got[k] = across(got[k - 1] if k == 3 else got[0], 2 if k == 2 else 1)
    far_keys = {}
    for k in far:
        low = k & -k
        far_keys[k] = across(far_keys[k - low] if k > low else keys, low)
        got[k + 1] = across(jnp.concatenate([got[k], far_keys[k]], axis=0), 1)
        far_keys[k + 1] = got[k + 1][tok:]

    far_keys.update((k, x[tok:]) for k, x in enumerate(got[:4]))
    split = max(5 * n_queue // 8, 1)
    pieces = {(0, 0): jnp.concatenate([far_keys[k] for k in range(split)], axis=0)}
    pieces[0, 1] = jnp.concatenate([far_keys[k] for k in range(split, n_queue)], axis=0)
    step = n_batch // 2
    while step:
        for (b, p), x in list(pieces.items()):
            k = step if p else step | 1
            pieces[b ^ k, p] = beside(x, k)
        step //= 2

    pairs = pairs_of(n_queue)
    part_shape = jax.ShapeDtypeStruct((3, 2 * tok), jnp.float32)
    queue_shape = jax.ShapeDtypeStruct(queue_keys.shape, queue_keys.dtype)
    first, pos = kernel_call(
        first_kernel,
        (opened, rate, pos_index.reshape(1, tok), got[0], got[1], queue_keys),
        [VMEM] * 6,
        (part_shape, jax.ShapeDtypeStruct((1, tok), jnp.float32)),
        (VMEM, VMEM),
        cost=cost,
    )
    parts = [first]
    for a, b in pairs[1:-1]:
        parts.append(
            kernel_call(middle_kernel, (rate, got[a], got[b], queue_keys), [VMEM] * 4, part_shape, VMEM, cost=cost)
        )
    stats_shape = jax.ShapeDtypeStruct((4 * n_queue, tok), jnp.float32)
    stats = kernel_call(
        functools.partial(last_kernel, pairs),
        (rate, got[pairs[-1][0]], got[pairs[-1][1]], queue_keys, pos, *parts),
        [VMEM] + [VMEM] * (4 + len(parts)),
        stats_shape,
        VMEM,
        [pltpu.VMEM((3, 2 * tok), jnp.float32)],
        cost=cost,
    )
    per_dev = queue_keys.shape[0] // BLOCK
    base = kernel_call(
        base_kernel, (first, queue_keys), [HBM, VMEM], queue_shape, HBM, [pltpu.SemaphoreType.DMA], cost=cost
    )
    k = 1
    while k < n_queue:
        came = across(stats, k)
        stats = kernel_call(merge_kernel, (rate, stats, came), [VMEM] * 3, stats_shape, VMEM)
        k *= 2
    loss, term = kernel_call(
        final_kernel,
        (rate, stats),
        [VMEM, VMEM],
        (jax.ShapeDtypeStruct((1, tok), jnp.float32), jax.ShapeDtypeStruct((1, tok), jnp.float32)),
        (VMEM, VMEM),
        [pltpu.VMEM((n_queue, tok), jnp.float32)],
    )
    terms = [term] + [beside(term, k) for k in range(n_batch - 1, 0, -1)]
    temp_grad = kernel_call(grad_kernel, terms, [VMEM] * n_batch, jax.ShapeDtypeStruct((1, 1), jnp.float32), VMEM)
    new_queue = kernel_call(
        functools.partial(enqueue_kernel, n_queue, n_batch, split, list(pieces)),
        (write_pointer, block_order, base, *pieces.values()),
        [SMEM, SMEM, HBM] + [VMEM] * len(pieces),
        queue_shape,
        HBM,
        [pltpu.SemaphoreType.DMA((per_dev,))],
        input_output_aliases={2: 0},
    )
    return (loss.reshape(tok), temp_grad.reshape(1), new_queue)


def solution(mesh):
    n_queue, n_batch = mesh.shape["queue"], mesh.shape["batch"]
    placed = (
        P(("queue", "batch"), None),
        P(("queue", "batch"), None),
        P("queue", None),
        P(),
        P(),
        P(),
        P(("queue", "batch")),
    )
    return jax.shard_map(
        functools.partial(per_device, n_queue, n_batch),
        mesh=mesh,
        in_specs=placed,
        out_specs=(P(("queue", "batch")), P(), P("queue", None)),
        check_vma=False,
    )
```

```python
import functools

import jax
import jax.numpy as jnp
from jax import lax
from jax.experimental import pallas as pl
from jax.experimental.pallas import tpu as pltpu
from jax.sharding import PartitionSpec as P


BLOCK = 128
TILE = 256
LOG2E = 1.4426950408889634
LARGE = 2.0**60
VMEM = pl.BlockSpec(memory_space=pltpu.VMEM)
HBM = pl.BlockSpec(memory_space=pltpu.HBM)
SMEM = pl.BlockSpec(memory_space=pltpu.SMEM)


def dot_t(a, b):
    return lax.dot_general(a, b, (((1,), (1,)), ((), ())), preferred_element_type=jnp.float32)


def scores_of(k_ref, q, t):
    return dot_t(k_ref[pl.ds(t * TILE, TILE), :], q).reshape(TILE // 8, 8, q.shape[0])


def settle(m, s, w, c, o_ref):
    top = jnp.max(m, axis=0, keepdims=True)
    a = jnp.exp2((m - top) * c)
    o_ref[0:1, :] = top
    o_ref[1:2, :] = jnp.sum(s * a, axis=0, keepdims=True)
    o_ref[2:3, :] = jnp.sum(w * a, axis=0, keepdims=True)


def accumulate(rate_ref, q, k_ref, o_ref):
    count, tiles = q.shape[0], k_ref.shape[0] // TILE
    c = jnp.concatenate([rate_ref[...]] * (count // rate_ref.shape[1]), axis=1) * LOG2E
    d = scores_of(k_ref, q, 0)
    m = jnp.max(d, axis=0)
    e = jnp.exp2((d - m[None]) * c[None])
    s = jnp.sum(e, axis=0)
    w = jnp.sum(e * d, axis=0)
    for t in range(1, tiles):
        d = scores_of(k_ref, q, t)
        e = jnp.exp2((d - m[None]) * c[None])
        s = s + jnp.sum(e, axis=0)
        w = w + jnp.sum(e * d, axis=0)
    settle(m, s, w, c, o_ref)

    @pl.when(jnp.logical_not(jnp.max(s) < LARGE))
    def _():
        def step(t, carry):
            m, s, w = carry
            d = scores_of(k_ref, q, t)
            higher = jnp.maximum(m, jnp.max(d, axis=0))
            a = jnp.exp2((m - higher) * c)
            e = jnp.exp2((d - higher[None]) * c[None])
            return higher, s * a + jnp.sum(e, axis=0), w * a + jnp.sum(e * d, axis=0)

        zero = jnp.zeros((8, count), jnp.float32)
        settle(*lax.fori_loop(0, tiles, step, (m, zero, zero)), c, o_ref)


def both(a_ref, b_ref, tok):
    return jnp.concatenate([a_ref[:tok, :], b_ref[:tok, :]], axis=0)


def open_kernel(o_ref):
    o_ref[...] = jnp.zeros_like(o_ref)


def first_kernel(_, __, rate_ref, index_ref, qa_ref, qb_ref, k_ref, o_ref, pos_ref):
    tok = qa_ref.shape[0] // 2
    scores = dot_t(qa_ref[tok:, :], qa_ref[:tok, :])
    rows = lax.broadcasted_iota(jnp.int32, scores.shape, 0)
    pos_ref[...] = jnp.sum(jnp.where(rows == index_ref[...], scores, 0.0), axis=0, keepdims=True)
    accumulate(rate_ref, both(qa_ref, qb_ref, tok), k_ref, o_ref)


def middle_kernel(rate_ref, qa_ref, qb_ref, k_ref, o_ref):
    accumulate(rate_ref, both(qa_ref, qb_ref, o_ref.shape[1] // 2), k_ref, o_ref)


def last_kernel(pairs, rate_ref, qa_ref, qb_ref, k_ref, pos_ref, *refs):
    *parts, o_ref, own = refs
    n, tok = o_ref.shape[0] // 4, o_ref.shape[1]
    me = lax.axis_index("queue")
    o_ref[3 * n :, :] = jnp.zeros((n, tok), jnp.float32)
    o_ref[pl.ds(3 * n + me, 1), :] = pos_ref[...]

    def lay(pair, part):
        for j, k in enumerate(pair):
            at = jnp.bitwise_xor(me, k)
            for i in range(3):
                o_ref[pl.ds(i * n + at, 1), :] = part[i : i + 1, j * tok : (j + 1) * tok]

    for pair, part in zip(pairs, parts):
        lay(pair, part)
    accumulate(rate_ref, both(qa_ref, qb_ref, tok), k_ref, own)
    lay(pairs[-1], own)


def merge_kernel(rate_ref, a_ref, b_ref, o_ref):
    n, tok = o_ref.shape[0] // 4, o_ref.shape[1]
    scale = jnp.broadcast_to(rate_ref[0:1, :], (n, tok))
    ours, theirs = a_ref[0:n, :], b_ref[0:n, :]
    level = jnp.maximum(ours, theirs)
    f, g = jnp.exp(scale * (ours - level)), jnp.exp(scale * (theirs - level))
    o_ref[0:n, :] = level
    o_ref[n : 2 * n, :] = a_ref[n : 2 * n, :] * f + b_ref[n : 2 * n, :] * g
    o_ref[2 * n : 3 * n, :] = a_ref[2 * n : 3 * n, :] * f + b_ref[2 * n : 3 * n, :] * g
    o_ref[3 * n :, :] = a_ref[3 * n :, :] + b_ref[3 * n :, :]


def base_kernel(_, ptr_ref, k_ref, base_ref, sem):
    copy = pltpu.make_async_copy(k_ref, base_ref, sem)
    copy.start()
    copy.wait()


def final_kernel(rate_ref, stats_ref, loss_ref, term_ref, hold_ref):
    n, tok = stats_ref.shape[0] // 4, stats_ref.shape[1]
    scale = jnp.broadcast_to(rate_ref[0:1, :], (n, tok))
    peak = scale * stats_ref[0:n, :]
    total = stats_ref[n : 2 * n, :]
    weighted = stats_ref[2 * n : 3 * n, :]
    pos = scale * stats_ref[3 * n :, :]
    highest = jnp.maximum(peak, pos)
    factor = jnp.exp(peak - highest)
    own = jnp.exp(pos - highest)
    final_total = total * factor + own
    final_weighted = scale * weighted * factor + pos * own
    hold_ref[...] = highest + jnp.log(final_total) - pos
    loss_ref[...] = hold_ref[pl.ds(lax.axis_index("queue"), 1), :]
    terms = final_weighted / final_total - pos
    mean = jnp.sum(terms, keepdims=True) / (n * tok * lax.axis_size("batch"))
    term_ref[...] = jnp.broadcast_to(mean, term_ref.shape)


def grad_kernel(*refs):
    *terms, o_ref = refs
    o_ref[...] = sum((x[0:1, 0:1] for x in terms[1:]), terms[0][0:1, 0:1])


def enqueue_kernel(n_queue, n_batch, split, held, ptr, block_order, base_ref, *refs):
    *pieces, out_ref, sem = refs
    per_dev = out_ref.shape[0] // BLOCK
    total = per_dev * n_queue
    count = block_order.shape[0]
    each = count // (n_queue * n_batch)
    me_q, me_b = lax.axis_index("queue"), lax.axis_index("batch")
    offset = ptr[0] - me_q * per_dev
    offset = jnp.where(offset < 0, offset + total, offset)

    def rows(i):
        return pl.ds(pl.multiple_of(i * BLOCK, BLOCK), BLOCK)

    def slot_of(c):
        at = offset + block_order[c]
        return jnp.where(at >= total, at - total, at)

    def start(b, p, piece, r, _):
        dq = r // each + (split if p else 0)
        dev = jnp.bitwise_xor(me_q, dq) * n_batch + jnp.bitwise_xor(me_b, b)
        slot = slot_of(dev * each + r % each)

        @pl.when(slot < per_dev)
        def _():
            pltpu.make_async_copy(piece.at[rows(r)], out_ref.at[rows(slot)], sem.at[slot]).start()

        return 0

    def finish(slot, _):
        pltpu.make_async_copy(pieces[0].at[rows(0)], out_ref.at[rows(slot)], sem.at[slot]).wait()
        return 0

    @pl.when((offset < per_dev) | (offset + count > total))
    def _():
        for (b, p), piece in zip(held, pieces):
            lax.fori_loop(0, piece.shape[0] // BLOCK, functools.partial(start, b, p, piece), 0)
        lax.fori_loop(jnp.minimum(offset, per_dev), jnp.minimum(offset + count, per_dev), finish, 0)
        lax.fori_loop(0, jnp.maximum(offset + count - total, 0), finish, 0)


def kernel_call(kernel, operands, specs, shapes, out_specs, scratch=(), cost=None, **more):
    return pl.pallas_call(
        kernel,
        out_shape=shapes,
        in_specs=specs,
        out_specs=out_specs,
        scratch_shapes=list(scratch),
        compiler_params=pltpu.CompilerParams(vmem_limit_bytes=12 << 20),
        cost_estimate=cost,
        **more,
    )(*operands)


def evens(n):
    return sorted(range(2, n, 2), key=lambda k: (bin(k).count("1"), -k))


def pairs_of(n):
    early, late = range(4, n, 2), range(5, n, 2)
    return [(0, 1), *zip(early[::2], early[1::2]), (2, 3), *zip(late[::2], late[1::2])]


def per_device(n_queue, n_batch, queries, keys, queue_keys, log_scale, write_pointer, block_order, pos_index):
    tok, width = queries.shape

    def hop(x, axis, n, k):
        return lax.ppermute(x, axis, [(i, i ^ k) for i in range(n)])

    def across(x, k):
        return hop(x, "queue", n_queue, k)

    def beside(x, k):
        return hop(x, "batch", n_batch, k)

    cost = pl.CostEstimate(
        flops=4 * tok * queue_keys.shape[0] * width,
        bytes_accessed=queue_keys.size * 2,
        transcendentals=2 * tok * queue_keys.shape[0],
    )
    rate = jnp.broadcast_to(jnp.exp(log_scale), (8, tok))
    wait = pl.CostEstimate(flops=64 * cost.flops, bytes_accessed=4096, transcendentals=0)
    gate = kernel_call(open_kernel, (), [], jax.ShapeDtypeStruct((8, 128), jnp.float32), VMEM)
    opened = kernel_call(open_kernel, (), [], jax.ShapeDtypeStruct((8, 128), jnp.float32), VMEM, cost=wait)

    got = [None] * n_queue
    far = [k for k in evens(n_queue) if k > 2]
    for k in far:
        low = k & -k
        got[k] = across(got[k - low] if k > low else queries, low)
    above = lax.broadcasted_iota(jnp.int32, (2 * tok, width), 0) < tok
    got[0] = jnp.where(above, jnp.pad(queries, ((0, tok), (0, 0))), jnp.pad(keys, ((tok, 0), (0, 0))))
    for k in (2, 1, 3):
        if k < n_queue:
            got[k] = across(got[k - 1] if k == 3 else got[0], 2 if k == 2 else 1)
    far_keys = {}
    for k in far:
        low = k & -k
        far_keys[k] = across(far_keys[k - low] if k > low else keys, low)
        got[k + 1] = across(jnp.concatenate([got[k], far_keys[k]], axis=0), 1)
        far_keys[k + 1] = got[k + 1][tok:]

    far_keys.update((k, x[tok:]) for k, x in enumerate(got[:4]))
    split = max(5 * n_queue // 8, 1)
    pieces = {(0, 0): jnp.concatenate([far_keys[k] for k in range(split)], axis=0)}
    pieces[0, 1] = jnp.concatenate([far_keys[k] for k in range(split, n_queue)], axis=0)
    step = n_batch // 2
    while step:
        for (b, p), x in list(pieces.items()):
            k = step if p else step | 1
            pieces[b ^ k, p] = beside(x, k)
        step //= 2

    pairs = pairs_of(n_queue)
    part_shape = jax.ShapeDtypeStruct((3, 2 * tok), jnp.float32)
    queue_shape = jax.ShapeDtypeStruct(queue_keys.shape, queue_keys.dtype)
    first, pos = kernel_call(
        first_kernel,
        (opened, gate, rate, pos_index.reshape(1, tok), got[0], got[1], queue_keys),
        [VMEM] * 7,
        (part_shape, jax.ShapeDtypeStruct((1, tok), jnp.float32)),
        (VMEM, VMEM),
        cost=cost,
    )
    parts = [first]
    for a, b in pairs[1:-1]:
        parts.append(
            kernel_call(middle_kernel, (rate, got[a], got[b], queue_keys), [VMEM] * 4, part_shape, VMEM, cost=cost)
        )
    stats_shape = jax.ShapeDtypeStruct((4 * n_queue, tok), jnp.float32)
    stats = kernel_call(
        functools.partial(last_kernel, pairs),
        (rate, got[pairs[-1][0]], got[pairs[-1][1]], queue_keys, pos, *parts),
        [VMEM] + [VMEM] * (4 + len(parts)),
        stats_shape,
        VMEM,
        [pltpu.VMEM((3, 2 * tok), jnp.float32)],
        cost=cost,
    )
    per_dev = queue_keys.shape[0] // BLOCK
    base = kernel_call(
        base_kernel, (first, write_pointer, queue_keys), [HBM, SMEM, VMEM], queue_shape, HBM, [pltpu.SemaphoreType.DMA], cost=cost
    )
    k = 1
    while k < n_queue:
        came = across(stats, k)
        stats = kernel_call(merge_kernel, (rate, stats, came), [VMEM] * 3, stats_shape, VMEM)
        k *= 2
    loss, term = kernel_call(
        final_kernel,
        (rate, stats),
        [VMEM, VMEM],
        (jax.ShapeDtypeStruct((1, tok), jnp.float32), jax.ShapeDtypeStruct((1, tok), jnp.float32)),
        (VMEM, VMEM),
        [pltpu.VMEM((n_queue, tok), jnp.float32)],
    )
    terms = [term] + [beside(term, k) for k in range(n_batch - 1, 0, -1)]
    temp_grad = kernel_call(grad_kernel, terms, [VMEM] * n_batch, jax.ShapeDtypeStruct((1, 1), jnp.float32), VMEM)
    new_queue = kernel_call(
        functools.partial(enqueue_kernel, n_queue, n_batch, split, list(pieces)),
        (write_pointer, block_order, base, *pieces.values()),
        [SMEM, SMEM, HBM] + [VMEM] * len(pieces),
        queue_shape,
        HBM,
        [pltpu.SemaphoreType.DMA((per_dev,))],
        input_output_aliases={2: 0},
    )
    return (loss.reshape(tok), temp_grad.reshape(1), new_queue)


def solution(mesh):
    n_queue, n_batch = mesh.shape["queue"], mesh.shape["batch"]
    placed = (
        P(("queue", "batch"), None),
        P(("queue", "batch"), None),
        P("queue", None),
        P(),
        P(),
        P(),
        P(("queue", "batch")),
    )
    return jax.shard_map(
        functools.partial(per_device, n_queue, n_batch),
        mesh=mesh,
        in_specs=placed,
        out_specs=(P(("queue", "batch")), P(), P("queue", None)),
        check_vma=False,
    )
```

```python
import functools

import jax
import jax.numpy as jnp
from jax import lax
from jax.experimental import pallas as pl
from jax.experimental.pallas import tpu as pltpu
from jax.sharding import PartitionSpec as P


BLOCK = 128
TILE = 256
LOG2E = 1.4426950408889634
LARGE = 2.0**60
VMEM = pl.BlockSpec(memory_space=pltpu.VMEM)
HBM = pl.BlockSpec(memory_space=pltpu.HBM)
SMEM = pl.BlockSpec(memory_space=pltpu.SMEM)


def dot_t(a, b):
    return lax.dot_general(a, b, (((1,), (1,)), ((), ())), preferred_element_type=jnp.float32)


def scores_of(k_ref, q, t):
    return dot_t(k_ref[pl.ds(t * TILE, TILE), :], q).reshape(TILE // 8, 8, q.shape[0])


def settle(m, s, w, c, o_ref):
    top = jnp.max(m, axis=0, keepdims=True)
    a = jnp.exp2((m - top) * c)
    o_ref[0:1, :] = top
    o_ref[1:2, :] = jnp.sum(s * a, axis=0, keepdims=True)
    o_ref[2:3, :] = jnp.sum(w * a, axis=0, keepdims=True)


def accumulate(rate_ref, q, k_ref, o_ref):
    count, tiles = q.shape[0], k_ref.shape[0] // TILE
    c = jnp.concatenate([rate_ref[...]] * (count // rate_ref.shape[1]), axis=1) * LOG2E
    d = scores_of(k_ref, q, 0)
    m = jnp.max(d, axis=0)
    e = jnp.exp2((d - m[None]) * c[None])
    s = jnp.sum(e, axis=0)
    w = jnp.sum(e * d, axis=0)
    for t in range(1, tiles):
        d = scores_of(k_ref, q, t)
        e = jnp.exp2((d - m[None]) * c[None])
        s = s + jnp.sum(e, axis=0)
        w = w + jnp.sum(e * d, axis=0)
    settle(m, s, w, c, o_ref)

    @pl.when(jnp.logical_not(jnp.max(s) < LARGE))
    def _():
        def step(t, carry):
            m, s, w = carry
            d = scores_of(k_ref, q, t)
            higher = jnp.maximum(m, jnp.max(d, axis=0))
            a = jnp.exp2((m - higher) * c)
            e = jnp.exp2((d - higher[None]) * c[None])
            return higher, s * a + jnp.sum(e, axis=0), w * a + jnp.sum(e * d, axis=0)

        zero = jnp.zeros((8, count), jnp.float32)
        settle(*lax.fori_loop(0, tiles, step, (m, zero, zero)), c, o_ref)


def both(a_ref, b_ref, tok):
    return jnp.concatenate([a_ref[:tok, :], b_ref[:tok, :]], axis=0)


def open_kernel(o_ref):
    o_ref[...] = jnp.zeros_like(o_ref)


def first_kernel(_, __, rate_ref, index_ref, qa_ref, qb_ref, k_ref, o_ref, pos_ref):
    tok = qa_ref.shape[0] // 2
    scores = dot_t(qa_ref[tok:, :], qa_ref[:tok, :])
    rows = lax.broadcasted_iota(jnp.int32, scores.shape, 0)
    pos_ref[...] = jnp.sum(jnp.where(rows == index_ref[...], scores, 0.0), axis=0, keepdims=True)
    accumulate(rate_ref, both(qa_ref, qb_ref, tok), k_ref, o_ref)


def middle_kernel(rate_ref, qa_ref, qb_ref, k_ref, o_ref):
    accumulate(rate_ref, both(qa_ref, qb_ref, o_ref.shape[1] // 2), k_ref, o_ref)


def last_kernel(pairs, rate_ref, qa_ref, qb_ref, k_ref, pos_ref, *refs):
    *parts, o_ref, own = refs
    n, tok = o_ref.shape[0] // 4, o_ref.shape[1]
    me = lax.axis_index("queue")
    o_ref[3 * n :, :] = jnp.zeros((n, tok), jnp.float32)
    o_ref[pl.ds(3 * n + me, 1), :] = pos_ref[...]

    def lay(pair, part):
        for j, k in enumerate(pair):
            at = jnp.bitwise_xor(me, k)
            for i in range(3):
                o_ref[pl.ds(i * n + at, 1), :] = part[i : i + 1, j * tok : (j + 1) * tok]

    for pair, part in zip(pairs, parts):
        lay(pair, part)
    accumulate(rate_ref, both(qa_ref, qb_ref, tok), k_ref, own)
    lay(pairs[-1], own)


def merge_kernel(rate_ref, a_ref, b_ref, o_ref):
    n, tok = o_ref.shape[0] // 4, o_ref.shape[1]
    scale = jnp.broadcast_to(rate_ref[0:1, :], (n, tok))
    ours, theirs = a_ref[0:n, :], b_ref[0:n, :]
    level = jnp.maximum(ours, theirs)
    f, g = jnp.exp(scale * (ours - level)), jnp.exp(scale * (theirs - level))
    o_ref[0:n, :] = level
    o_ref[n : 2 * n, :] = a_ref[n : 2 * n, :] * f + b_ref[n : 2 * n, :] * g
    o_ref[2 * n : 3 * n, :] = a_ref[2 * n : 3 * n, :] * f + b_ref[2 * n : 3 * n, :] * g
    o_ref[3 * n :, :] = a_ref[3 * n :, :] + b_ref[3 * n :, :]


def base_kernel(_, ptr_ref, k_ref, base_ref, sem):
    copy = pltpu.make_async_copy(k_ref, base_ref, sem)
    copy.start()
    copy.wait()


def final_kernel(rate_ref, stats_ref, loss_ref, term_ref, hold_ref):
    n, tok = stats_ref.shape[0] // 4, stats_ref.shape[1]
    scale = jnp.broadcast_to(rate_ref[0:1, :], (n, tok))
    peak = scale * stats_ref[0:n, :]
    total = stats_ref[n : 2 * n, :]
    weighted = stats_ref[2 * n : 3 * n, :]
    pos = scale * stats_ref[3 * n :, :]
    highest = jnp.maximum(peak, pos)
    factor = jnp.exp(peak - highest)
    own = jnp.exp(pos - highest)
    final_total = total * factor + own
    final_weighted = scale * weighted * factor + pos * own
    hold_ref[...] = highest + jnp.log(final_total) - pos
    loss_ref[...] = hold_ref[pl.ds(lax.axis_index("queue"), 1), :]
    terms = final_weighted / final_total - pos
    mean = jnp.sum(terms, keepdims=True) / (n * tok * lax.axis_size("batch"))
    term_ref[...] = jnp.broadcast_to(mean, term_ref.shape)


def grad_kernel(*refs):
    *terms, o_ref = refs
    o_ref[...] = sum((x[0:1, 0:1] for x in terms[1:]), terms[0][0:1, 0:1])


def enqueue_kernel(n_queue, n_batch, split, held, ptr, block_order, base_ref, *refs):
    *pieces, out_ref, sem = refs
    per_dev = out_ref.shape[0] // BLOCK
    total = per_dev * n_queue
    count = block_order.shape[0]
    each = count // (n_queue * n_batch)
    me_q, me_b = lax.axis_index("queue"), lax.axis_index("batch")
    offset = ptr[0] - me_q * per_dev
    offset = jnp.where(offset < 0, offset + total, offset)

    def rows(i):
        return pl.ds(pl.multiple_of(i * BLOCK, BLOCK), BLOCK)

    def slot_of(c):
        at = offset + block_order[c]
        return jnp.where(at >= total, at - total, at)

    def start(b, p, piece, r, _):
        dq = r // each + (split if p else 0)
        dev = jnp.bitwise_xor(me_q, dq) * n_batch + jnp.bitwise_xor(me_b, b)
        slot = slot_of(dev * each + r % each)

        @pl.when(slot < per_dev)
        def _():
            pltpu.make_async_copy(piece.at[rows(r)], out_ref.at[rows(slot)], sem.at[slot]).start()

        return 0

    def finish(slot, _):
        pltpu.make_async_copy(pieces[0].at[rows(0)], out_ref.at[rows(slot)], sem.at[slot]).wait()
        return 0

    @pl.when((offset < per_dev) | (offset + count > total))
    def _():
        for (b, p), piece in zip(held, pieces):
            lax.fori_loop(0, piece.shape[0] // BLOCK, functools.partial(start, b, p, piece), 0)
        lax.fori_loop(jnp.minimum(offset, per_dev), jnp.minimum(offset + count, per_dev), finish, 0)
        lax.fori_loop(0, jnp.maximum(offset + count - total, 0), finish, 0)


def kernel_call(kernel, operands, specs, shapes, out_specs, scratch=(), cost=None, **more):
    return pl.pallas_call(
        kernel,
        out_shape=shapes,
        in_specs=specs,
        out_specs=out_specs,
        scratch_shapes=list(scratch),
        compiler_params=pltpu.CompilerParams(vmem_limit_bytes=12 << 20),
        cost_estimate=cost,
        **more,
    )(*operands)


def evens(n):
    return sorted(range(2, n, 2), key=lambda k: (bin(k).count("1"), -k))


def pairs_of(n):
    early, late = range(4, n, 2), range(5, n, 2)
    return [(0, 1), *zip(early[::2], early[1::2]), (2, 3), *zip(late[::2], late[1::2])]


def per_device(n_queue, n_batch, queries, keys, queue_keys, log_scale, write_pointer, block_order, pos_index):
    tok, width = queries.shape

    def hop(x, axis, n, k):
        return lax.ppermute(x, axis, [(i, i ^ k) for i in range(n)])

    def across(x, k):
        return hop(x, "queue", n_queue, k)

    def beside(x, k):
        return hop(x, "batch", n_batch, k)

    cost = pl.CostEstimate(
        flops=4 * tok * queue_keys.shape[0] * width,
        bytes_accessed=queue_keys.size * 2,
        transcendentals=2 * tok * queue_keys.shape[0],
    )
    rate = jnp.broadcast_to(jnp.exp(log_scale), (8, tok))
    wait = pl.CostEstimate(flops=64 * cost.flops, bytes_accessed=4096, transcendentals=0)
    gate = kernel_call(open_kernel, (), [], jax.ShapeDtypeStruct((8, 128), jnp.float32), VMEM)
    opened = kernel_call(open_kernel, (), [], jax.ShapeDtypeStruct((8, 128), jnp.float32), VMEM, cost=wait)

    got = [None] * n_queue
    far = [k for k in evens(n_queue) if k > 2]
    for k in far:
        low = k & -k
        got[k] = across(got[k - low] if k > low else queries, low)
    above = lax.broadcasted_iota(jnp.int32, (2 * tok, width), 0) < tok
    got[0] = jnp.where(above, jnp.pad(queries, ((0, tok), (0, 0))), jnp.pad(keys, ((tok, 0), (0, 0))))
    for k in (2, 1, 3):
        if k < n_queue:
            got[k] = across(got[k - 1] if k == 3 else got[0], 2 if k == 2 else 1)
    far_keys = {}
    for k in far:
        low = k & -k
        far_keys[k] = across(far_keys[k - low] if k > low else keys, low)
        got[k + 1] = across(got[k], 1)
    if far:
        odd = across(jnp.concatenate([far_keys[k] for k in far], axis=0), 1)
        far_keys.update((k + 1, odd[i * tok : (i + 1) * tok]) for i, k in enumerate(far))

    far_keys.update((k, x[tok:]) for k, x in enumerate(got[:4]))
    split = max(5 * n_queue // 8, 1)
    pieces = {(0, 0): jnp.concatenate([far_keys[k] for k in range(split)], axis=0)}
    pieces[0, 1] = jnp.concatenate([far_keys[k] for k in range(split, n_queue)], axis=0)
    step = n_batch // 2
    while step:
        for (b, p), x in list(pieces.items()):
            k = step if p else step | 1
            pieces[b ^ k, p] = beside(x, k)
        step //= 2

    pairs = pairs_of(n_queue)
    part_shape = jax.ShapeDtypeStruct((3, 2 * tok), jnp.float32)
    queue_shape = jax.ShapeDtypeStruct(queue_keys.shape, queue_keys.dtype)
    first, pos = kernel_call(
        first_kernel,
        (opened, gate, rate, pos_index.reshape(1, tok), got[0], got[1], queue_keys),
        [VMEM] * 7,
        (part_shape, jax.ShapeDtypeStruct((1, tok), jnp.float32)),
        (VMEM, VMEM),
        cost=cost,
    )
    parts = [first]
    for a, b in pairs[1:-1]:
        parts.append(
            kernel_call(middle_kernel, (rate, got[a], got[b], queue_keys), [VMEM] * 4, part_shape, VMEM, cost=cost)
        )
    stats_shape = jax.ShapeDtypeStruct((4 * n_queue, tok), jnp.float32)
    stats = kernel_call(
        functools.partial(last_kernel, pairs),
        (rate, got[pairs[-1][0]], got[pairs[-1][1]], queue_keys, pos, *parts),
        [VMEM] + [VMEM] * (4 + len(parts)),
        stats_shape,
        VMEM,
        [pltpu.VMEM((3, 2 * tok), jnp.float32)],
        cost=cost,
    )
    per_dev = queue_keys.shape[0] // BLOCK
    base = kernel_call(
        base_kernel, (first, write_pointer, queue_keys), [HBM, SMEM, VMEM], queue_shape, HBM, [pltpu.SemaphoreType.DMA], cost=cost
    )
    k = 1
    while k < n_queue:
        came = across(stats, k)
        stats = kernel_call(merge_kernel, (rate, stats, came), [VMEM] * 3, stats_shape, VMEM)
        k *= 2
    loss, term = kernel_call(
        final_kernel,
        (rate, stats),
        [VMEM, VMEM],
        (jax.ShapeDtypeStruct((1, tok), jnp.float32), jax.ShapeDtypeStruct((1, tok), jnp.float32)),
        (VMEM, VMEM),
        [pltpu.VMEM((n_queue, tok), jnp.float32)],
    )
    terms = [term] + [beside(term, k) for k in range(n_batch - 1, 0, -1)]
    temp_grad = kernel_call(grad_kernel, terms, [VMEM] * n_batch, jax.ShapeDtypeStruct((1, 1), jnp.float32), VMEM)
    new_queue = kernel_call(
        functools.partial(enqueue_kernel, n_queue, n_batch, split, list(pieces)),
        (write_pointer, block_order, base, *pieces.values()),
        [SMEM, SMEM, HBM] + [VMEM] * len(pieces),
        queue_shape,
        HBM,
        [pltpu.SemaphoreType.DMA((per_dev,))],
        input_output_aliases={2: 0},
    )
    return (loss.reshape(tok), temp_grad.reshape(1), new_queue)


def solution(mesh):
    n_queue, n_batch = mesh.shape["queue"], mesh.shape["batch"]
    placed = (
        P(("queue", "batch"), None),
        P(("queue", "batch"), None),
        P("queue", None),
        P(),
        P(),
        P(),
        P(("queue", "batch")),
    )
    return jax.shard_map(
        functools.partial(per_device, n_queue, n_batch),
        mesh=mesh,
        in_specs=placed,
        out_specs=(P(("queue", "batch")), P(), P("queue", None)),
        check_vma=False,
    )
```
